128 devices in a mesh: row: 2 (over core), col: 64 (over z, y, x).
Axes of the slice: x: 4, y: 4, z: 4, core: 2. Of those that a mesh axis runs over, the one named last changes fastest.
Arguments:
- w_one: float32 [2, 64, 2, 128, 512], P('row', 'col')
- w_two: float32 [2, 64, 2, 512, 128], P('row', 'col')
- inputs: bfloat16 [2, 64, 3, 2048, 128], P('row', 'col')
- targets: bfloat16 [2, 64, 3, 2048, 128], P('row', 'col')
Outputs:
- output 1: float32 [2, 64, 2, 128, 512], P('row', 'col')
- output 2: float32 [2, 64, 2, 512, 128], P('row', 'col')
All inputs are finite; a program needn't handle non-finite values.
Results may differ from the reference program's by a relative error of at most 0.00126359.
Values are sent between devices in bfloat16 or wider.
A program may use at most 1 GiB of HBM per device.

```python
import jax
import jax.numpy as jnp
from jax import lax

GRID_ROWS = 2
GRID_COLS = 64
LAYERS = 2
NUM_STEPS = 3
BATCH_ROWS = 2048
D_MODEL = 128
D_FF = 512

LEARN_RATE = 1.5
NORM_EPS = 1e-6
GELU_C = 0.7978845608028654
GELU_K = 0.044715
REPLICA_SPREAD = 0.5


def gelu_value(pre_act):
    tanh_inner = jnp.tanh(GELU_C * (pre_act + GELU_K * pre_act * pre_act * pre_act))
    return 0.5 * pre_act * (1.0 + tanh_inner)


def gelu_slope(pre_act):
    tanh_inner = jnp.tanh(GELU_C * (pre_act + GELU_K * pre_act * pre_act * pre_act))
    return 0.5 * (1.0 + tanh_inner) + 0.5 * pre_act * (1.0 - tanh_inner * tanh_inner) * GELU_C * (1.0 + 3.0 * GELU_K * pre_act * pre_act)


def setup_inputs(seed: int = 0) -> dict:
    root_key = jax.random.key(seed)
    sub_keys = jax.random.split(root_key, 6)
    grid_shape = (GRID_ROWS, GRID_COLS)
    shape_one = (LAYERS, D_MODEL, D_FF)
    shape_two = (LAYERS, D_FF, D_MODEL)
    norm_fac = (1.0 + REPLICA_SPREAD * REPLICA_SPREAD) ** -0.5
    base_one = jax.random.normal(sub_keys[0], shape_one, jnp.float32)
    own_one = jax.random.normal(sub_keys[1], grid_shape + shape_one, jnp.float32)
    w_one = (base_one + REPLICA_SPREAD * own_one) * (norm_fac * D_MODEL ** -0.5)
    base_two = jax.random.normal(sub_keys[2], shape_two, jnp.float32)
    own_two = jax.random.normal(sub_keys[3], grid_shape + shape_two, jnp.float32)
    w_two = (base_two + REPLICA_SPREAD * own_two) * (norm_fac * D_FF ** -0.5)
    data_shape = grid_shape + (NUM_STEPS, BATCH_ROWS, D_MODEL)
    inputs = jax.random.normal(sub_keys[4], data_shape, jnp.float32).astype(jnp.bfloat16)
    targets = jax.random.normal(sub_keys[5], data_shape, jnp.float32).astype(jnp.bfloat16)
    return {'w_one': w_one, 'w_two': w_two, 'inputs': inputs, 'targets': targets}


def local_update(w_one, w_two, x_in, target):
    one_lo = w_one.astype(jnp.bfloat16)
    two_lo = w_two.astype(jnp.bfloat16)
    hidden = x_in
    saved_acts = []
    for layer_idx in range(LAYERS):
        hid_f = hidden.astype(jnp.float32)
        inv_rms = lax.rsqrt(jnp.mean(hid_f * hid_f, axis=-1, keepdims=True) + NORM_EPS)
        normed = hid_f * inv_rms
        normed_lo = normed.astype(jnp.bfloat16)
        pre_act = jnp.dot(normed_lo, one_lo[layer_idx], preferred_element_type=jnp.float32)
        act_lo = gelu_value(pre_act).astype(jnp.bfloat16)
        mlp_out = jnp.dot(act_lo, two_lo[layer_idx], preferred_element_type=jnp.float32)
        saved_acts.append((normed, inv_rms, normed_lo, pre_act, act_lo))
        hidden = (hid_f + mlp_out).astype(jnp.bfloat16)
    d_hidden = (2.0 / (BATCH_ROWS * D_MODEL)) * (hidden.astype(jnp.float32) - target.astype(jnp.float32))
    grads_one = [None] * LAYERS
    grads_two = [None] * LAYERS
    for layer_idx in reversed(range(LAYERS)):
        normed, inv_rms, normed_lo, pre_act, act_lo = saved_acts[layer_idx]
        d_lo = d_hidden.astype(jnp.bfloat16)
        grads_two[layer_idx] = jnp.dot(act_lo.T, d_lo, preferred_element_type=jnp.float32)
        d_act = jnp.dot(d_lo, two_lo[layer_idx].T, preferred_element_type=jnp.float32)
        d_pre = (d_act * gelu_slope(pre_act)).astype(jnp.bfloat16)
        grads_one[layer_idx] = jnp.dot(normed_lo.T, d_pre, preferred_element_type=jnp.float32)
        if layer_idx > 0:
            d_normed = jnp.dot(d_pre, one_lo[layer_idx].T, preferred_element_type=jnp.float32)
            d_hidden = d_hidden + inv_rms * (d_normed - normed * jnp.mean(d_normed * normed, axis=-1, keepdims=True))
    return w_one - LEARN_RATE * jnp.stack(grads_one), w_two - LEARN_RATE * jnp.stack(grads_two)


def gossip_mix(upd_vals):
    wire_vals = upd_vals.astype(jnp.bfloat16)
    mix_sum = upd_vals + jnp.roll(wire_vals, 1, axis=1).astype(jnp.float32)
    mix_sum = mix_sum + jnp.roll(wire_vals, -1, axis=1).astype(jnp.float32)
    mix_sum = mix_sum + jnp.roll(wire_vals, 1, axis=0).astype(jnp.float32)
    mix_sum = mix_sum + jnp.roll(wire_vals, -1, axis=0).astype(jnp.float32)
    return mix_sum / 5.0


def reference(w_one, w_two, inputs, targets):
    n_rep = GRID_ROWS * GRID_COLS
    for step_idx in range(NUM_STEPS):
        flat_one = w_one.reshape((n_rep, LAYERS, D_MODEL, D_FF))
        flat_two = w_two.reshape((n_rep, LAYERS, D_FF, D_MODEL))
        x_step = inputs[:, :, step_idx].reshape((n_rep, BATCH_ROWS, D_MODEL))
        t_step = targets[:, :, step_idx].reshape((n_rep, BATCH_ROWS, D_MODEL))
        upd_one, upd_two = lax.map(lambda packed: local_update(packed[0], packed[1], packed[2], packed[3]), (flat_one, flat_two, x_step, t_step))
        w_one = gossip_mix(upd_one.reshape(w_one.shape))
        w_two = gossip_mix(upd_two.reshape(w_two.shape))
    return w_one, w_two
```

```python
import functools

import jax
import jax.numpy as jnp
from jax import lax
from jax.experimental import pallas as pl
from jax.experimental.pallas import tpu as pltpu
from jax.sharding import PartitionSpec as P

LEARN_RATE = 1.5
NORM_EPS = 1e-6
GELU_C = 0.7978845608028654
GELU_K = 0.044715
MESH = pl.DeviceIdType.MESH
F32 = jnp.float32
BF16 = jnp.bfloat16
N_DEST = 3
N_PART = 2


def dot(lhs, rhs):
    return lax.dot_general(lhs, rhs, (((1,), (0,)), ((), ())), preferred_element_type=F32)


def dot_rhs_t(lhs, rhs):
    return lax.dot_general(lhs, rhs, (((1,), (1,)), ((), ())), preferred_element_type=F32)


def gelu_and_slope(z):
    cubic = (GELU_C * GELU_K * z) * z
    th = jnp.tanh(z * (GELU_C + cubic))
    half = 0.5 + 0.5 * th
    act = z * half
    slope = half + act * (1.0 - th) * (GELU_C + 3.0 * cubic)
    return act, slope


def kernel(n_rows, n_cols, w1_hbm, w2_hbm, x_hbm, t_hbm, o1_hbm, o2_hbm,
           xs, ts, w2_in, master, wlo, act, slope, n_lo, n_tr, inv_b, hid, err, err_lo, err_tr, grad_a, grad_b,
           send, recv, in_sem, out_sem, send_sem, recv_sem):
    n_steps, batch, width = xs.shape
    hidden = act.shape[2]
    part = hidden // N_PART
    row, col = lax.axis_index("row"), lax.axis_index("col")
    nxt, prv = lax.rem(col + 1, n_cols), lax.rem(col + n_cols - 1, n_cols)
    dests = ((row, nxt), (row, prv), (lax.rem(row + 1, n_rows), col))

    def start(src, dst, idx):
        cp = pltpu.make_async_copy(src, dst, in_sem.at[idx])
        cp.start()
        return cp

    cp_x, cp_t = [None] * n_steps, [None] * n_steps
    cp_x[0] = start(x_hbm.at[0], xs.at[0], 0)
    cp_w1 = [start(w1_hbm.at[l], master.at[2 * l], 1 + l) for l in range(2)]
    cp_w2 = [start(w2_hbm.at[l], w2_in.at[l], 3 + l) for l in range(2)]
    for t in range(n_steps):
        if t:
            cp_x[t] = start(x_hbm.at[t], xs.at[t], 4 + 2 * t)
        cp_t[t] = start(t_hbm.at[t], ts.at[t], 5 + 2 * t)

    barrier = pltpu.get_barrier_semaphore()
    for dest in dests:
        pl.semaphore_signal(barrier, inc=1, device_id=dest, device_id_type=MESH)

    def over_rows(size, body, unroll=1):
        def step(i, carry):
            body(pl.ds(pl.multiple_of(i * size, size), size))
            return carry
        lax.fori_loop(0, batch // size, step, 0, unroll=unroll)

    def norm_of(x):
        return lax.rsqrt(jnp.mean(x * x, axis=-1, keepdims=True) + NORM_EPS)

    def prepare(t):
        def body(rows):
            x = xs[t, rows, :].astype(F32)
            n = (x * norm_of(x)).astype(BF16)
            n_lo[0, rows, :] = n
            n_tr[0, :, rows] = n.T
        over_rows(512, body)

    def hidden_phase(l, cols, sub=128):
        def body(rows):
            for s in range(rows.size // sub):
                r = pl.ds(rows.start + s * sub, sub)
                a, d = gelu_and_slope(dot(n_lo[l, r, :], wlo[2 * l, :, cols]))
                act[l, r, cols] = a.astype(BF16)
                slope[l, r, cols] = d
        over_rows(512, body)

    def out0_phase(t):
        def body(rows):
            o = dot_rhs_t(act[0, rows, :], wlo[1])
            h = (xs[t, rows, :].astype(F32) + o).astype(BF16)
            hid[rows, :] = h
            x = h.astype(F32)
            inv = norm_of(x)
            n = (x * inv).astype(BF16)
            inv_b[rows, :] = jnp.broadcast_to(inv, x.shape)
            n_lo[1, rows, :] = n
            n_tr[1, :, rows] = n.T
        over_rows(512, body)

    def out1_phase(t):
        loss_scale = 2.0 / (batch * width)

        def body(rows):
            o = dot_rhs_t(act[1, rows, :], wlo[3])
            h = (hid[rows, :].astype(F32) + o).astype(BF16)
            e = loss_scale * (h.astype(F32) - ts[t, rows, :].astype(F32))
            lo = e.astype(BF16)
            err[rows, :] = e
            err_lo[rows, :] = lo
            err_tr[:, rows] = lo.T
        over_rows(512, body)

    def update(t, u, grad):
        q = master[u] - LEARN_RATE * grad
        master[u] = q
        lo = q.astype(BF16)
        for h in range(N_PART):
            send[t, u * N_PART + h] = lo[:, h * part:(h + 1) * part]

    def copy_of(t, d, k):
        return pltpu.make_async_remote_copy(
            src_ref=send.at[t, k], dst_ref=recv.at[t, d, k], send_sem=send_sem.at[t, d, k],
            recv_sem=recv_sem.at[t, d, k], device_id=dests[d], device_id_type=MESH)

    def push(t, *ks):
        for k in ks:
            for d in range(N_DEST):
                copy_of(t, d, k).start()

    def combine(t, k):
        for d in range(N_DEST):
            copy_of(t, d, k).wait_recv()
        u, h = divmod(k, N_PART)
        cols = slice(h * part, (h + 1) * part)
        other = recv[t, 2, k].astype(F32)
        total = master[u, :, cols] + recv[t, 0, k].astype(F32) + recv[t, 1, k].astype(F32) + other + other
        p = total / 5.0
        master[u, :, cols] = p
        if t < n_steps - 1:
            wlo[u, :, cols] = p.astype(BF16)

    def back1_phase():
        grad_a[...] = jnp.zeros_like(grad_a)
        grad_b[...] = jnp.zeros_like(grad_b)

        def body(rows):
            d_act = dot(err_lo[rows, :], wlo[3])
            dz = (d_act * slope[1, rows, :]).astype(BF16)
            grad_a[...] += dot(n_tr[1, :, rows], dz)
            m = dot_rhs_t(dz, wlo[2])
            inv = inv_b[rows, :]
            n = hid[rows, :].astype(F32) * inv
            e = err[rows, :] + inv * (m - n * jnp.mean(m * n, axis=-1, keepdims=True))
            lo = e.astype(BF16)
            err_lo[rows, :] = lo
            grad_b[...] += dot(lo.T, act[0, rows, :])
        over_rows(512, body)

    def back0_phase():
        grad_a[...] = jnp.zeros_like(grad_a)

        def body(rows):
            d_act = dot(err_lo[rows, :], wlo[1])
            dz = (d_act * slope[0, rows, :]).astype(BF16)
            grad_a[...] += dot(n_tr[0, :, rows], dz)
        over_rows(512, body)

    halves = [slice(h * part, (h + 1) * part) for h in range(N_PART)]
    cp_x[0].wait()
    prepare(0)
    for l in range(2):
        cp_w1[l].wait()
        wlo[2 * l] = master[2 * l].astype(BF16)
    for l in range(2):
        cp_w2[l].wait()
        w = w2_in[l].T
        master[2 * l + 1] = w
        wlo[2 * l + 1] = w.astype(BF16)

    for t in range(n_steps):
        for h in range(N_PART):
            if t:
                combine(t - 1, h)
            hidden_phase(0, halves[h])
        if t:
            combine(t - 1, 2)
            combine(t - 1, 3)
        out0_phase(t)
        for h in range(N_PART):
            if t:
                combine(t - 1, 4 + h)
            hidden_phase(1, halves[h])
        cp_t[t].wait()
        if t:
            combine(t - 1, 6)
            combine(t - 1, 7)
        out1_phase(t)
        update(t, 3, dot(err_tr[...], act[1]))
        if t == 0:
            pl.semaphore_wait(barrier, N_DEST)
        push(t, 6, 7)
        back1_phase()
        update(t, 2, grad_a[...])
        update(t, 1, grad_b[...])
        back0_phase()
        update(t, 0, grad_a[...])
        push(t, 0, 1, 2, 3, 4, 5)
        if t < n_steps - 1:
            cp_x[t + 1].wait()
            prepare(t + 1)

    last = n_steps - 1
    outs = []
    for u in (3, 0, 1, 2):
        l = u // 2
        for h in range(N_PART):
            combine(last, u * N_PART + h)
        if u % 2:
            w2_in[l] = master[u].T
            cp = pltpu.make_async_copy(w2_in.at[l], o2_hbm.at[l], out_sem.at[u])
        else:
            cp = pltpu.make_async_copy(master.at[u], o1_hbm.at[l], out_sem.at[u])
        cp.start()
        outs.append(cp)
    for t in range(n_steps):
        for d in range(N_DEST):
            for k in range(4 * N_PART):
                copy_of(t, d, k).wait_send()
    for cp in outs:
        cp.wait()


def solution(mesh):
    n_rows, n_cols = mesh.shape["row"], mesh.shape["col"]

    def device_fn(w_one, w_two, inputs, targets):
        layers, width, hidden = w_one.shape[2:]
        steps, batch, _ = inputs.shape[2:]
        n_piece = 2 * layers * N_PART
        part = hidden // N_PART
        anywhere = pl.BlockSpec(memory_space=pl.ANY)
        o1, o2 = pl.pallas_call(
            functools.partial(kernel, n_rows, n_cols),
            out_shape=(jax.ShapeDtypeStruct((layers, width, hidden), F32), jax.ShapeDtypeStruct((layers, hidden, width), F32)),
            in_specs=[anywhere] * 4,
            out_specs=(anywhere, anywhere),
            scratch_shapes=[
                pltpu.VMEM((steps, batch, width), BF16),
                pltpu.VMEM((steps, batch, width), BF16),
                pltpu.VMEM((layers, hidden, width), F32),
                pltpu.VMEM((2 * layers, width, hidden), F32),
                pltpu.VMEM((2 * layers, width, hidden), BF16),
                pltpu.VMEM((layers, batch, hidden), BF16),
                pltpu.VMEM((layers, batch, hidden), F32),
                pltpu.VMEM((layers, batch, width), BF16),
                pltpu.VMEM((layers, width, batch), BF16),
                pltpu.VMEM((batch, width), F32),
                pltpu.VMEM((batch, width), BF16),
                pltpu.VMEM((batch, width), F32),
                pltpu.VMEM((batch, width), BF16),
                pltpu.VMEM((width, batch), BF16),
                pltpu.VMEM((width, hidden), F32),
                pltpu.VMEM((width, hidden), F32),
                pltpu.VMEM((steps, n_piece, width, part), BF16),
                pltpu.VMEM((steps, N_DEST, n_piece, width, part), BF16),
                pltpu.SemaphoreType.DMA((5 + 2 * steps,)),
                pltpu.SemaphoreType.DMA((2 * layers,)),
                pltpu.SemaphoreType.DMA((steps, N_DEST, n_piece)),
                pltpu.SemaphoreType.DMA((steps, N_DEST, n_piece)),
            ],
            compiler_params=pltpu.CompilerParams(collective_id=0, has_side_effects=True, vmem_limit_bytes=60 * 1024 * 1024),
        )(w_one[0, 0], w_two[0, 0], inputs[0, 0], targets[0, 0])
        return o1[None, None], o2[None, None]

    grid_spec = P("row", "col")
    return jax.shard_map(device_fn, mesh=mesh, in_specs=(grid_spec,) * 4, out_specs=(grid_spec, grid_spec), check_vma=False)
```

```python
import functools

import jax
import jax.numpy as jnp
from jax import lax
from jax.experimental import pallas as pl
from jax.experimental.pallas import tpu as pltpu
from jax.sharding import PartitionSpec as P

LEARN_RATE = 1.5
NORM_EPS = 1e-6
GELU_C = 0.7978845608028654
GELU_K = 0.044715
MESH = pl.DeviceIdType.MESH
F32 = jnp.float32
BF16 = jnp.bfloat16
N_DEST = 3
N_PART = 2


def dot(lhs, rhs):
    return lax.dot_general(lhs, rhs, (((1,), (0,)), ((), ())), preferred_element_type=F32)


def dot_rhs_t(lhs, rhs):
    return lax.dot_general(lhs, rhs, (((1,), (1,)), ((), ())), preferred_element_type=F32)


def gelu_and_slope(z):
    cubic = (GELU_C * GELU_K * z) * z
    th = jnp.tanh(z * (GELU_C + cubic))
    half = 0.5 + 0.5 * th
    act = z * half
    slope = half + act * (1.0 - th) * (GELU_C + 3.0 * cubic)
    return act, slope


def kernel(n_rows, n_cols, w1_hbm, w2_hbm, x_hbm, t_hbm, o1_hbm, o2_hbm,
           xs, ts, w2_in, master, wlo, act, slope, n_lo, n_tr, inv_b, hid, err, err_lo, err_tr, dz,
           send, recv, in_sem, out_sem, send_sem, recv_sem):
    n_steps, batch, width = xs.shape
    hidden = act.shape[2]
    part = hidden // N_PART
    row, col = lax.axis_index("row"), lax.axis_index("col")
    nxt, prv = lax.rem(col + 1, n_cols), lax.rem(col + n_cols - 1, n_cols)
    dests = ((row, nxt), (row, prv), (lax.rem(row + 1, n_rows), col))

    def start(src, dst, idx):
        cp = pltpu.make_async_copy(src, dst, in_sem.at[idx])
        cp.start()
        return cp

    cp_x, cp_t = [None] * n_steps, [None] * n_steps
    cp_x[0] = start(x_hbm.at[0], xs.at[0], 0)
    cp_w1 = [start(w1_hbm.at[l], master.at[2 * l], 1 + l) for l in range(2)]
    cp_w2 = [start(w2_hbm.at[l], w2_in.at[l], 3 + l) for l in range(2)]
    for t in range(n_steps):
        if t:
            cp_x[t] = start(x_hbm.at[t], xs.at[t], 4 + 2 * t)
        cp_t[t] = start(t_hbm.at[t], ts.at[t], 5 + 2 * t)

    barrier = pltpu.get_barrier_semaphore()
    for dest in dests:
        pl.semaphore_signal(barrier, inc=1, device_id=dest, device_id_type=MESH)

    def blocks(size):
        return [slice(i, i + size) for i in range(0, batch, size)]

    def norm_of(x):
        return lax.rsqrt(jnp.mean(x * x, axis=-1, keepdims=True) + NORM_EPS)

    def prepare(t):
        for rows in blocks(256):
            x = xs[t, rows, :].astype(F32)
            n = (x * norm_of(x)).astype(BF16)
            n_lo[0, rows, :] = n
            n_tr[0, :, rows] = n.T

    def hidden_phase(l, cols):
        for rows in blocks(128):
            a, d = gelu_and_slope(dot(n_lo[l, rows, :], wlo[2 * l, :, cols]))
            act[l, rows, cols] = a.astype(BF16)
            slope[l, rows, cols] = d

    def out0_phase(t):
        for rows in blocks(256):
            o = dot_rhs_t(act[0, rows, :], wlo[1])
            h = (xs[t, rows, :].astype(F32) + o).astype(BF16)
            hid[rows, :] = h
            x = h.astype(F32)
            inv = norm_of(x)
            n = (x * inv).astype(BF16)
            inv_b[rows, :] = jnp.broadcast_to(inv, x.shape)
            n_lo[1, rows, :] = n
            n_tr[1, :, rows] = n.T

    def out1_phase(t):
        loss_scale = 2.0 / (batch * width)
        for rows in blocks(256):
            o = dot_rhs_t(act[1, rows, :], wlo[3])
            h = (hid[rows, :].astype(F32) + o).astype(BF16)
            e = loss_scale * (h.astype(F32) - ts[t, rows, :].astype(F32))
            lo = e.astype(BF16)
            err[rows, :] = e
            err_lo[rows, :] = lo
            err_tr[:, rows] = lo.T

    def d_pre_phase(l):
        for rows in blocks(512):
            d_act = dot(err_lo[rows, :], wlo[2 * l + 1])
            dz[rows, :] = (d_act * slope[l, rows, :]).astype(BF16)

    def d_hidden_phase():
        for rows in blocks(512):
            m = dot_rhs_t(dz[rows, :], wlo[2])
            inv = inv_b[rows, :]
            n = hid[rows, :].astype(F32) * inv
            e = err[rows, :] + inv * (m - n * jnp.mean(m * n, axis=-1, keepdims=True))
            lo = e.astype(BF16)
            err_lo[rows, :] = lo
            err_tr[:, rows] = lo.T

    def update(t, u, grad):
        q = master[u] - LEARN_RATE * grad
        master[u] = q
        lo = q.astype(BF16)
        for h in range(N_PART):
            send[t, u * N_PART + h] = lo[:, h * part:(h + 1) * part]

    def copy_of(t, d, k):
        return pltpu.make_async_remote_copy(
            src_ref=send.at[t, k], dst_ref=recv.at[t, d, k], send_sem=send_sem.at[t, d, k],
            recv_sem=recv_sem.at[t, d, k], device_id=dests[d], device_id_type=MESH)

    def push(t, *ks):
        for k in ks:
            for d in range(N_DEST):
                copy_of(t, d, k).start()

    def combine(t, k):
        for d in range(N_DEST):
            copy_of(t, d, k).wait_recv()
        u, h = divmod(k, N_PART)
        cols = slice(h * part, (h + 1) * part)
        other = recv[t, 2, k].astype(F32)
        total = master[u, :, cols] + recv[t, 0, k].astype(F32) + recv[t, 1, k].astype(F32) + other + other
        p = total / 5.0
        master[u, :, cols] = p
        if t < n_steps - 1:
            wlo[u, :, cols] = p.astype(BF16)

    halves = [slice(h * part, (h + 1) * part) for h in range(N_PART)]
    cp_x[0].wait()
    prepare(0)
    for l in range(2):
        cp_w1[l].wait()
        wlo[2 * l] = master[2 * l].astype(BF16)
    for l in range(2):
        cp_w2[l].wait()
        w = w2_in[l].T
        master[2 * l + 1] = w
        wlo[2 * l + 1] = w.astype(BF16)

    for t in range(n_steps):
        for h in range(N_PART):
            if t:
                combine(t - 1, h)
            hidden_phase(0, halves[h])
        if t:
            combine(t - 1, 2)
            combine(t - 1, 3)
        out0_phase(t)
        for h in range(N_PART):
            if t:
                combine(t - 1, 4 + h)
            hidden_phase(1, halves[h])
        cp_t[t].wait()
        if t:
            combine(t - 1, 6)
            combine(t - 1, 7)
        out1_phase(t)
        update(t, 3, dot(err_tr[...], act[1]))
        if t == 0:
            pl.semaphore_wait(barrier, N_DEST)
        push(t, 6)
        d_pre_phase(1)
        update(t, 2, dot(n_tr[1], dz[...]))
        push(t, 4)
        d_hidden_phase()
        d_pre_phase(0)
        update(t, 0, dot(n_tr[0], dz[...]))
        push(t, 0, 1)
        update(t, 1, dot(err_tr[...], act[0]))
        push(t, 2, 3, 5, 7)
        if t < n_steps - 1:
            cp_x[t + 1].wait()
            prepare(t + 1)

    last = n_steps - 1
    outs = []
    for u in (0, 1, 2, 3):
        l = u // 2
        for h in range(N_PART):
            combine(last, u * N_PART + h)
        if u % 2:
            w2_in[l] = master[u].T
            cp = pltpu.make_async_copy(w2_in.at[l], o2_hbm.at[l], out_sem.at[u])
        else:
            cp = pltpu.make_async_copy(master.at[u], o1_hbm.at[l], out_sem.at[u])
        cp.start()
        outs.append(cp)
    for t in range(n_steps):
        for d in range(N_DEST):
            for k in range(4 * N_PART):
                copy_of(t, d, k).wait_send()
    for cp in outs:
        cp.wait()


def solution(mesh):
    n_rows, n_cols = mesh.shape["row"], mesh.shape["col"]

    def device_fn(w_one, w_two, inputs, targets):
        layers, width, hidden = w_one.shape[2:]
        steps, batch, _ = inputs.shape[2:]
        n_piece = 2 * layers * N_PART
        part = hidden // N_PART
        anywhere = pl.BlockSpec(memory_space=pl.ANY)
        o1, o2 = pl.pallas_call(
            functools.partial(kernel, n_rows, n_cols),
            out_shape=(jax.ShapeDtypeStruct((layers, width, hidden), F32), jax.ShapeDtypeStruct((layers, hidden, width), F32)),
            in_specs=[anywhere] * 4,
            out_specs=(anywhere, anywhere),
            scratch_shapes=[
                pltpu.VMEM((steps, batch, width), BF16),
                pltpu.VMEM((steps, batch, width), BF16),
                pltpu.VMEM((layers, hidden, width), F32),
                pltpu.VMEM((2 * layers, width, hidden), F32),
                pltpu.VMEM((2 * layers, width, hidden), BF16),
                pltpu.VMEM((layers, batch, hidden), BF16),
                pltpu.VMEM((layers, batch, hidden), F32),
                pltpu.VMEM((layers, batch, width), BF16),
                pltpu.VMEM((layers, width, batch), BF16),
                pltpu.VMEM((batch, width), F32),
                pltpu.VMEM((batch, width), BF16),
                pltpu.VMEM((batch, width), F32),
                pltpu.VMEM((batch, width), BF16),
                pltpu.VMEM((width, batch), BF16),
                pltpu.VMEM((batch, hidden), BF16),
                pltpu.VMEM((steps, n_piece, width, part), BF16),
                pltpu.VMEM((steps, N_DEST, n_piece, width, part), BF16),
                pltpu.SemaphoreType.DMA((5 + 2 * steps,)),
                pltpu.SemaphoreType.DMA((2 * layers,)),
                pltpu.SemaphoreType.DMA((steps, N_DEST, n_piece)),
                pltpu.SemaphoreType.DMA((steps, N_DEST, n_piece)),
            ],
            compiler_params=pltpu.CompilerParams(collective_id=0, has_side_effects=True, vmem_limit_bytes=60 * 1024 * 1024),
        )(w_one[0, 0], w_two[0, 0], inputs[0, 0], targets[0, 0])
        return o1[None, None], o2[None, None]

    grid_spec = P("row", "col")
    return jax.shard_map(device_fn, mesh=mesh, in_specs=(grid_spec,) * 4, out_specs=(grid_spec, grid_spec), check_vma=False)
```

```python
import functools

import jax
import jax.numpy as jnp
from jax import lax
from jax.experimental import pallas as pl
from jax.experimental.pallas import tpu as pltpu
from jax.sharding import PartitionSpec as P

LEARN_RATE = 1.5
NORM_EPS = 1e-6
GELU_C = 0.7978845608028654
GELU_K = 0.044715
MESH = pl.DeviceIdType.MESH
F32 = jnp.float32
BF16 = jnp.bfloat16
N_DEST = 3
N_PART = 4


def dot(lhs, rhs):
    return lax.dot_general(lhs, rhs, (((1,), (0,)), ((), ())), preferred_element_type=F32)


def dot_rhs_t(lhs, rhs):
    return lax.dot_general(lhs, rhs, (((1,), (1,)), ((), ())), preferred_element_type=F32)


def gelu_and_slope(z):
    cubic = (GELU_C * GELU_K * z) * z
    th = jnp.tanh(z * (GELU_C + cubic))
    half = 0.5 + 0.5 * th
    act = z * half
    slope = half + act * (1.0 - th) * (GELU_C + 3.0 * cubic)
    return act, slope


def gelu_value(z):
    return z * (0.5 + 0.5 * jnp.tanh(z * (GELU_C + (GELU_C * GELU_K * z) * z)))


def kernel(n_rows, n_cols, w1_hbm, w2_hbm, x_hbm, t_hbm, o1, o2,
           xs, ts, w2_in, master, wlo, act, slope, n_lo, n_tr, inv_b, hid, err, err_lo, err_tr, dz,
           send, recv, in_sem, send_sem, recv_sem):
    n_steps, batch, width = xs.shape
    hidden = act.shape[2]
    part, half = hidden // N_PART, hidden // 2
    halves = [slice(0, half), slice(half, hidden)]
    row, col = lax.axis_index("row"), lax.axis_index("col")
    nxt, prv = lax.rem(col + 1, n_cols), lax.rem(col + n_cols - 1, n_cols)
    dests = ((row, nxt), (row, prv), (lax.rem(row + 1, n_rows), col))

    def start(src, dst, idx):
        cp = pltpu.make_async_copy(src, dst, in_sem.at[idx])
        cp.start()
        return cp

    cp_x, cp_t = [None] * n_steps, [None] * n_steps
    cp_x[0] = start(x_hbm.at[0], xs.at[0], 0)
    cp_w1 = [start(w1_hbm.at[l], master.at[2 * l], 1 + l) for l in range(2)]
    cp_w2 = [start(w2_hbm.at[l], w2_in.at[l], 3 + l) for l in range(2)]
    for t in range(n_steps):
        if t:
            cp_x[t] = start(x_hbm.at[t], xs.at[t], 4 + 2 * t)
        cp_t[t] = start(t_hbm.at[t], ts.at[t], 5 + 2 * t)

    barrier = pltpu.get_barrier_semaphore()
    for dest in dests:
        pl.semaphore_signal(barrier, inc=1, device_id=dest, device_id_type=MESH)

    def blocks(size):
        return [slice(i, i + size) for i in range(0, batch, size)]

    def norm_of(x):
        return lax.rsqrt(jnp.mean(x * x, axis=-1, keepdims=True) + NORM_EPS)

    def prepare(t):
        for rows in blocks(256):
            x = xs[t, rows, :].astype(F32)
            n_lo[0, rows, :] = (x * norm_of(x)).astype(BF16)

    def prepare_tr():
        for rows in blocks(256):
            n_tr[0, :, rows] = n_lo[0, rows, :].T

    def hidden_phase(l, cols, late):
        for rows in blocks(128):
            z = dot(n_lo[l, rows, :], wlo[2 * l, :, cols])
            if late:
                a, d = gelu_value(z), z
            else:
                a, d = gelu_and_slope(z)
            act[l, rows, cols] = a.astype(BF16)
            slope[l, rows, cols] = d

    def first_half(l, partial):
        for rows in blocks(256):
            partial[rows, :] = dot_rhs_t(act[l, rows, halves[0]], wlo[2 * l + 1, :, halves[0]])

    def product(l, rows, partial):
        if partial is None:
            return dot_rhs_t(act[l, rows, :], wlo[2 * l + 1])
        return partial[rows, :] + dot_rhs_t(act[l, rows, halves[1]], wlo[2 * l + 1, :, halves[1]])

    def out0_phase(t, partial):
        for rows in blocks(256):
            h = (xs[t, rows, :].astype(F32) + product(0, rows, partial)).astype(BF16)
            hid[rows, :] = h
            x = h.astype(F32)
            inv = norm_of(x)
            n = (x * inv).astype(BF16)
            inv_b[rows, :] = jnp.broadcast_to(inv, x.shape)
            n_lo[1, rows, :] = n
            n_tr[1, :, rows] = n.T

    def out1_phase(t, partial):
        loss_scale = 2.0 / (batch * width)
        for rows in blocks(256):
            h = (hid[rows, :].astype(F32) + product(1, rows, partial)).astype(BF16)
            e = loss_scale * (h.astype(F32) - ts[t, rows, :].astype(F32))
            lo = e.astype(BF16)
            err[rows, :] = e
            err_lo[rows, :] = lo
            err_tr[:, rows] = lo.T

    def d_pre_phase(l, late):
        for rows in blocks(512):
            d_act = dot(err_lo[rows, :], wlo[2 * l + 1])
            d = slope[l, rows, :]
            if late:
                d = gelu_and_slope(d)[1]
            dz[rows, :] = (d_act * d).astype(BF16)

    def d_hidden_phase():
        for rows in blocks(512):
            m = dot_rhs_t(dz[rows, :], wlo[2])
            inv = inv_b[rows, :]
            n = hid[rows, :].astype(F32) * inv
            e = err[rows, :] + inv * (m - n * jnp.mean(m * n, axis=-1, keepdims=True))
            lo = e.astype(BF16)
            err_lo[rows, :] = lo
            err_tr[:, rows] = lo.T

    def update(t, u, left, right, cols):
        q = master[u, :, cols] - LEARN_RATE * dot(left[...], right[:, cols])
        master[u, :, cols] = q
        lo = q.astype(BF16)
        for j in range(0, q.shape[1], part):
            send[t, u * N_PART + (cols.start + j) // part] = lo[:, j:j + part]

    def copy_of(t, d, k):
        return pltpu.make_async_remote_copy(
            src_ref=send.at[t, k], dst_ref=recv.at[t, d, k], send_sem=send_sem.at[t, d, k],
            recv_sem=recv_sem.at[t, d, k], device_id=dests[d], device_id_type=MESH)

    def push(t, u, *hs):
        for h in hs:
            for d in range(N_DEST):
                copy_of(t, d, u * N_PART + h).start()

    def combine(t, u, *hs):
        for h in hs:
            k = u * N_PART + h
            for d in range(N_DEST):
                copy_of(t, d, k).wait_recv()
            cols = slice(h * part, (h + 1) * part)
            other = recv[t, 2, k].astype(F32)
            total = master[u, :, cols] + recv[t, 0, k].astype(F32) + recv[t, 1, k].astype(F32) + other + other
            p = total / 5.0
            if t < n_steps - 1:
                master[u, :, cols] = p
                wlo[u, :, cols] = p.astype(BF16)
            elif u % 2:
                o2[u // 2, cols, :] = p.T
            else:
                o1[u // 2, :, cols] = p

    everything = slice(0, hidden)
    cp_x[0].wait()
    prepare(0)
    for l in range(2):
        cp_w1[l].wait()
        wlo[2 * l] = master[2 * l].astype(BF16)
    for l in range(2):
        cp_w2[l].wait()
        w = w2_in[l].T
        master[2 * l + 1] = w
        wlo[2 * l + 1] = w.astype(BF16)

    for t in range(n_steps):
        first = t == 0
        if first:
            hidden_phase(0, everything, True)
            out0_phase(t, None)
            hidden_phase(1, everything, False)
            cp_t[t].wait()
            out1_phase(t, None)
        else:
            combine(t - 1, 0, 0, 1)
            hidden_phase(0, halves[0], False)
            combine(t - 1, 0, 2, 3)
            hidden_phase(0, halves[1], False)
            combine(t - 1, 1, 0, 1)
            first_half(0, inv_b)
            combine(t - 1, 1, 2, 3)
            out0_phase(t, inv_b)
            combine(t - 1, 2, 0, 1)
            hidden_phase(1, halves[0], False)
            combine(t - 1, 3, 0, 1)
            first_half(1, err)
            combine(t - 1, 2, 2, 3)
            hidden_phase(1, halves[1], False)
            cp_t[t].wait()
            combine(t - 1, 3, 2, 3)
            out1_phase(t, err)
        update(t, 3, err_tr, act.at[1], halves[0])
        if first:
            pl.semaphore_wait(barrier, N_DEST)
        push(t, 3, 0, 1)
        update(t, 3, err_tr, act.at[1], halves[1])
        d_pre_phase(1, False)
        update(t, 2, n_tr.at[1], dz, everything)
        push(t, 2, 0, 1, 2)
        if first:
            prepare_tr()
        d_hidden_phase()
        d_pre_phase(0, first)
        update(t, 0, n_tr.at[0], dz, everything)
        push(t, 0, 0, 1, 2, 3)
        update(t, 1, err_tr, act.at[0], everything)
        push(t, 1, 0, 1, 2, 3)
        push(t, 2, 3)
        push(t, 3, 2, 3)
        if t < n_steps - 1:
            cp_x[t + 1].wait()
            prepare(t + 1)
            prepare_tr()

    last = n_steps - 1
    combine(last, 3, 0, 1)
    combine(last, 2, 0, 1, 2)
    combine(last, 0, 0, 1, 2, 3)
    combine(last, 1, 0, 1, 2, 3)
    combine(last, 2, 3)
    combine(last, 3, 2, 3)
    for t in range(n_steps):
        for d in range(N_DEST):
            for k in range(4 * N_PART):
                copy_of(t, d, k).wait_send()


def solution(mesh):
    n_rows, n_cols = mesh.shape["row"], mesh.shape["col"]

    def device_fn(w_one, w_two, inputs, targets):
        layers, width, hidden = w_one.shape[2:]
        steps, batch, _ = inputs.shape[2:]
        n_piece = 2 * layers * N_PART
        part = hidden // N_PART
        in_spec = pl.BlockSpec(memory_space=pltpu.HBM)
        out_spec = pl.BlockSpec(memory_space=pltpu.VMEM)
        o1, o2 = pl.pallas_call(
            functools.partial(kernel, n_rows, n_cols),
            out_shape=(jax.ShapeDtypeStruct((layers, width, hidden), F32), jax.ShapeDtypeStruct((layers, hidden, width), F32)),
            in_specs=[in_spec] * 4,
            out_specs=(out_spec, out_spec),
            scratch_shapes=[
                pltpu.VMEM((steps, batch, width), BF16),
                pltpu.VMEM((steps, batch, width), BF16),
                pltpu.VMEM((layers, hidden, width), F32),
                pltpu.VMEM((2 * layers, width, hidden), F32),
                pltpu.VMEM((2 * layers, width, hidden), BF16),
                pltpu.VMEM((layers, batch, hidden), BF16),
                pltpu.VMEM((layers, batch, hidden), F32),
                pltpu.VMEM((layers, batch, width), BF16),
                pltpu.VMEM((layers, width, batch), BF16),
                pltpu.VMEM((batch, width), F32),
                pltpu.VMEM((batch, width), BF16),
                pltpu.VMEM((batch, width), F32),
                pltpu.VMEM((batch, width), BF16),
                pltpu.VMEM((width, batch), BF16),
                pltpu.VMEM((batch, hidden), BF16),
                pltpu.VMEM((steps, n_piece, width, part), BF16),
                pltpu.VMEM((steps, N_DEST, n_piece, width, part), BF16),
                pltpu.SemaphoreType.DMA((5 + 2 * steps,)),
                pltpu.SemaphoreType.DMA((steps, N_DEST, n_piece)),
                pltpu.SemaphoreType.DMA((steps, N_DEST, n_piece)),
            ],
            compiler_params=pltpu.CompilerParams(collective_id=0, has_side_effects=True, vmem_limit_bytes=48 * 1024 * 1024),
        )(*[pltpu.with_memory_space_constraint(v[0, 0], pltpu.HBM) for v in (w_one, w_two, inputs, targets)])
        return o1[None, None], o2[None, None]

    grid_spec = P("row", "col")
    return jax.shard_map(device_fn, mesh=mesh, in_specs=(grid_spec,) * 4, out_specs=(grid_spec, grid_spec), check_vma=False)
```

```python
import functools

import jax
import jax.numpy as jnp
from jax import lax
from jax.experimental import pallas as pl
from jax.experimental.pallas import tpu as pltpu
from jax.sharding import PartitionSpec as P

LEARN_RATE = 1.5
NORM_EPS = 1e-6
GELU_C = 0.7978845608028654
GELU_K = 0.044715
MESH = pl.DeviceIdType.MESH
F32 = jnp.float32
BF16 = jnp.bfloat16
N_DEST = 3
N_PART = 4


def dot(lhs, rhs):
    return lax.dot_general(lhs, rhs, (((1,), (0,)), ((), ())), preferred_element_type=F32)


def dot_rhs_t(lhs, rhs):
    return lax.dot_general(lhs, rhs, (((1,), (1,)), ((), ())), preferred_element_type=F32)


def gelu_and_slope(z):
    cubic = (GELU_C * GELU_K * z) * z
    th = jnp.tanh(z * (GELU_C + cubic))
    half = 0.5 + 0.5 * th
    act = z * half
    slope = half + act * (1.0 - th) * (GELU_C + 3.0 * cubic)
    return act, slope


def gelu_value(z):
    return z * (0.5 + 0.5 * jnp.tanh(z * (GELU_C + (GELU_C * GELU_K * z) * z)))


def kernel(n_rows, n_cols, w1_hbm, w2_hbm, x_hbm, t_hbm, o1, o2,
           xs, ts, w2_in, master, wlo, act, slope, n_lo, n_tr, inv_b, hid, err, err_lo, err_tr, dz,
           send, recv, in_sem, send_sem, recv_sem):
    n_steps, batch, width = xs.shape
    hidden = act.shape[2]
    part, half = hidden // N_PART, hidden // 2
    halves = [slice(0, half), slice(half, hidden)]
    row, col = lax.axis_index("row"), lax.axis_index("col")
    nxt, prv = lax.rem(col + 1, n_cols), lax.rem(col + n_cols - 1, n_cols)
    dests = ((row, nxt), (row, prv), (lax.rem(row + 1, n_rows), col))

    def start(src, dst, idx):
        cp = pltpu.make_async_copy(src, dst, in_sem.at[idx])
        cp.start()
        return cp

    cp_x, cp_t = [None] * n_steps, [None] * n_steps
    cp_x[0] = start(x_hbm.at[0], xs.at[0], 0)
    cp_w1 = [start(w1_hbm.at[l], master.at[2 * l], 1 + l) for l in range(2)]
    cp_w2 = [start(w2_hbm.at[l], w2_in.at[l], 3 + l) for l in range(2)]
    for t in range(n_steps):
        if t:
            cp_x[t] = start(x_hbm.at[t], xs.at[t], 4 + 2 * t)
        cp_t[t] = start(t_hbm.at[t], ts.at[t], 5 + 2 * t)

    barrier = pltpu.get_barrier_semaphore()
    for dest in dests:
        pl.semaphore_signal(barrier, inc=1, device_id=dest, device_id_type=MESH)

    def blocks(size):
        return [slice(i, i + size) for i in range(0, batch, size)]

    def norm_of(x):
        return lax.rsqrt(jnp.mean(x * x, axis=-1, keepdims=True) + NORM_EPS)

    def prepare(t):
        for rows in blocks(256):
            x = xs[t, rows, :].astype(F32)
            n_lo[0, rows, :] = (x * norm_of(x)).astype(BF16)

    def prepare_tr():
        for rows in blocks(256):
            n_tr[0, :, rows] = n_lo[0, rows, :].T

    def hidden_phase(l, cols, late):
        for rows in blocks(128):
            z = dot(n_lo[l, rows, :], wlo[2 * l, :, cols])
            if late:
                a, d = gelu_value(z), z
            else:
                a, d = gelu_and_slope(z)
            act[l, rows, cols] = a.astype(BF16)
            slope[l, rows, cols] = d

    def first_half(l, partial):
        for rows in blocks(256):
            partial[rows, :] = dot_rhs_t(act[l, rows, halves[0]], wlo[2 * l + 1, :, halves[0]])

    def product(l, rows, partial):
        if partial is None:
            return dot_rhs_t(act[l, rows, :], wlo[2 * l + 1])
        return partial[rows, :] + dot_rhs_t(act[l, rows, halves[1]], wlo[2 * l + 1, :, halves[1]])

    def out0_phase(t, partial):
        for rows in blocks(256):
            h = (xs[t, rows, :].astype(F32) + product(0, rows, partial)).astype(BF16)
            hid[rows, :] = h
            x = h.astype(F32)
            inv = norm_of(x)
            n = (x * inv).astype(BF16)
            inv_b[rows, :] = jnp.broadcast_to(inv, x.shape)
            n_lo[1, rows, :] = n
            n_tr[1, :, rows] = n.T

    def out1_phase(t, partial):
        loss_scale = 2.0 / (batch * width)
        for rows in blocks(256):
            h = (hid[rows, :].astype(F32) + product(1, rows, partial)).astype(BF16)
            e = loss_scale * (h.astype(F32) - ts[t, rows, :].astype(F32))
            lo = e.astype(BF16)
            err[rows, :] = e
            err_lo[rows, :] = lo
            err_tr[1, :, rows] = lo.T

    def d_pre_phase(l, cols, late):
        for rows in blocks(512):
            d_act = dot(err_lo[rows, :], wlo[2 * l + 1, :, cols])
            d = slope[l, rows, cols]
            if late:
                d = gelu_and_slope(d)[1]
            dz[l, rows, cols] = (d_act * d).astype(BF16)

    def d_hidden_phase():
        for rows in blocks(512):
            m = dot_rhs_t(dz[1, rows, :], wlo[2])
            inv = inv_b[rows, :]
            n = hid[rows, :].astype(F32) * inv
            e = err[rows, :] + inv * (m - n * jnp.mean(m * n, axis=-1, keepdims=True))
            lo = e.astype(BF16)
            err_lo[rows, :] = lo
            err_tr[0, :, rows] = lo.T

    def update(t, u, left, right, cols):
        q = master[u, :, cols] - LEARN_RATE * dot(left[...], right[:, cols])
        master[u, :, cols] = q
        lo = q.astype(BF16)
        for j in range(0, q.shape[1], part):
            send[t, u * N_PART + (cols.start + j) // part] = lo[:, j:j + part]

    def copy_of(t, d, k):
        return pltpu.make_async_remote_copy(
            src_ref=send.at[t, k], dst_ref=recv.at[t, d, k], send_sem=send_sem.at[t, d, k],
            recv_sem=recv_sem.at[t, d, k], device_id=dests[d], device_id_type=MESH)

    def push(t, u, *hs):
        for h in hs:
            for d in range(N_DEST):
                copy_of(t, d, u * N_PART + h).start()

    def combine(t, u, *hs):
        for h in hs:
            k = u * N_PART + h
            for d in range(N_DEST):
                copy_of(t, d, k).wait_recv()
            cols = slice(h * part, (h + 1) * part)
            other = recv[t, 2, k].astype(F32)
            total = master[u, :, cols] + recv[t, 0, k].astype(F32) + recv[t, 1, k].astype(F32) + other + other
            p = total / 5.0
            if t < n_steps - 1:
                master[u, :, cols] = p
                wlo[u, :, cols] = p.astype(BF16)
            elif u % 2:
                o2[u // 2, cols, :] = p.T
            else:
                o1[u // 2, :, cols] = p

    everything = slice(0, hidden)
    cp_x[0].wait()
    prepare(0)
    for l in range(2):
        cp_w1[l].wait()
        wlo[2 * l] = master[2 * l].astype(BF16)
    for l in range(2):
        cp_w2[l].wait()
        w = w2_in[l].T
        master[2 * l + 1] = w
        wlo[2 * l + 1] = w.astype(BF16)

    for t in range(n_steps):
        first = t == 0
        if first:
            hidden_phase(0, everything, True)
            out0_phase(t, None)
            hidden_phase(1, everything, False)
            cp_t[t].wait()
            out1_phase(t, None)
        else:
            combine(t - 1, 3, 0, 1)
            combine(t - 1, 2, 0, 1)
            combine(t - 1, 0, 0, 1)
            hidden_phase(0, halves[0], False)
            combine(t - 1, 0, 2, 3)
            hidden_phase(0, halves[1], False)
            combine(t - 1, 1, 0, 1)
            first_half(0, inv_b)
            combine(t - 1, 1, 2, 3)
            out0_phase(t, inv_b)
            hidden_phase(1, halves[0], False)
            combine(t - 1, 2, 2, 3)
            hidden_phase(1, halves[1], False)
            cp_t[t].wait()
            combine(t - 1, 3, 2, 3)
            out1_phase(t, None)
        update(t, 3, err_tr.at[1], act.at[1], halves[0])
        if first:
            pl.semaphore_wait(barrier, N_DEST)
        push(t, 3, 0, 1)
        d_pre_phase(1, everything, False)
        update(t, 2, n_tr.at[1], dz.at[1], halves[0])
        push(t, 2, 0, 1)
        d_hidden_phase()
        if first:
            prepare_tr()
        d_pre_phase(0, halves[0], first)
        update(t, 0, n_tr.at[0], dz.at[0], halves[0])
        push(t, 0, 0, 1)
        d_pre_phase(0, halves[1], first)
        update(t, 0, n_tr.at[0], dz.at[0], halves[1])
        push(t, 0, 2, 3)
        update(t, 1, err_tr.at[0], act.at[0], everything)
        push(t, 1, 0, 1, 2, 3)
        update(t, 2, n_tr.at[1], dz.at[1], halves[1])
        push(t, 2, 2, 3)
        update(t, 3, err_tr.at[1], act.at[1], halves[1])
        push(t, 3, 2, 3)
        if t < n_steps - 1:
            cp_x[t + 1].wait()
            prepare(t + 1)
            prepare_tr()

    last = n_steps - 1
    combine(last, 3, 0, 1)
    combine(last, 2, 0, 1)
    combine(last, 0, 0, 1, 2, 3)
    combine(last, 1, 0, 1, 2, 3)
    combine(last, 2, 2, 3)
    combine(last, 3, 2, 3)
    for t in range(n_steps):
        for d in range(N_DEST):
            for k in range(4 * N_PART):
                copy_of(t, d, k).wait_send()


def solution(mesh):
    n_rows, n_cols = mesh.shape["row"], mesh.shape["col"]

    def device_fn(w_one, w_two, inputs, targets):
        layers, width, hidden = w_one.shape[2:]
        steps, batch, _ = inputs.shape[2:]
        n_piece = 2 * layers * N_PART
        part = hidden // N_PART
        in_spec = pl.BlockSpec(memory_space=pltpu.HBM)
        out_spec = pl.BlockSpec(memory_space=pltpu.VMEM)
        o1, o2 = pl.pallas_call(
            functools.partial(kernel, n_rows, n_cols),
            out_shape=(jax.ShapeDtypeStruct((layers, width, hidden), F32), jax.ShapeDtypeStruct((layers, hidden, width), F32)),
            in_specs=[in_spec] * 4,
            out_specs=(out_spec, out_spec),
            scratch_shapes=[
                pltpu.VMEM((steps, batch, width), BF16),
                pltpu.VMEM((steps, batch, width), BF16),
                pltpu.VMEM((layers, hidden, width), F32),
                pltpu.VMEM((2 * layers, width, hidden), F32),
                pltpu.VMEM((2 * layers, width, hidden), BF16),
                pltpu.VMEM((layers, batch, hidden), BF16),
                pltpu.VMEM((layers, batch, hidden), F32),
                pltpu.VMEM((layers, batch, width), BF16),
                pltpu.VMEM((layers, width, batch), BF16),
                pltpu.VMEM((batch, width), F32),
                pltpu.VMEM((batch, width), BF16),
                pltpu.VMEM((batch, width), F32),
                pltpu.VMEM((batch, width), BF16),
                pltpu.VMEM((layers, width, batch), BF16),
                pltpu.VMEM((layers, batch, hidden), BF16),
                pltpu.VMEM((steps, n_piece, width, part), BF16),
                pltpu.VMEM((steps, N_DEST, n_piece, width, part), BF16),
                pltpu.SemaphoreType.DMA((5 + 2 * steps,)),
                pltpu.SemaphoreType.DMA((steps, N_DEST, n_piece)),
                pltpu.SemaphoreType.DMA((steps, N_DEST, n_piece)),
            ],
            compiler_params=pltpu.CompilerParams(collective_id=0, has_side_effects=True, vmem_limit_bytes=48 * 1024 * 1024),
        )(*[pltpu.with_memory_space_constraint(v[0, 0], pltpu.HBM) for v in (w_one, w_two, inputs, targets)])
        return o1[None, None], o2[None, None]

    grid_spec = P("row", "col")
    return jax.shard_map(device_fn, mesh=mesh, in_specs=(grid_spec,) * 4, out_specs=(grid_spec, grid_spec), check_vma=False)
```

```python
import functools

import jax
import jax.numpy as jnp
from jax import lax
from jax.experimental import pallas as pl
from jax.experimental.pallas import tpu as pltpu
from jax.sharding import PartitionSpec as P

LEARN_RATE = 1.5
NORM_EPS = 1e-6
GELU_C = 0.7978845608028654
GELU_K = 0.044715
MESH = pl.DeviceIdType.MESH
F32 = jnp.float32
BF16 = jnp.bfloat16
N_DEST = 3
SKEW = 256
N_PART = 2


def dot(lhs, rhs):
    return lax.dot_general(lhs, rhs, (((1,), (0,)), ((), ())), preferred_element_type=F32)


def dot_rhs_t(lhs, rhs):
    return lax.dot_general(lhs, rhs, (((1,), (1,)), ((), ())), preferred_element_type=F32)


def gelu_and_slope(z):
    cubic = (GELU_C * GELU_K * z) * z
    th = jnp.tanh(z * (GELU_C + cubic))
    half = 0.5 + 0.5 * th
    act = z * half
    slope = half + act * (1.0 - th) * (GELU_C + 3.0 * cubic)
    return act, slope


def gelu_value(z):
    return z * (0.5 + 0.5 * jnp.tanh(z * (GELU_C + (GELU_C * GELU_K * z) * z)))


def kernel(n_rows, n_cols, w1_hbm, w2_hbm, x_hbm, t_hbm, o1, o2,
           xs, ts, w2_in, master, wlo, act, slope, n_lo, n_tr, inv_b, hid, err, err_lo, err_tr, dz,
           send, recv, in_sem, send_sem, recv_sem):
    n_steps, batch, width = xs.shape
    hidden = act.shape[2]
    part, half = hidden // N_PART, hidden // 2
    halves = [slice(0, half), slice(half, hidden)]
    row, col = lax.axis_index("row"), lax.axis_index("col")
    nxt, prv = lax.rem(col + 1, n_cols), lax.rem(col + n_cols - 1, n_cols)
    dests = ((row, nxt), (row, prv), (lax.rem(row + 1, n_rows), col))

    def start(src, dst, idx):
        cp = pltpu.make_async_copy(src, dst, in_sem.at[idx])
        cp.start()
        return cp

    cp_w1 = [None] * 2
    cp_w1[0] = start(w1_hbm.at[0], master.at[0], 0)
    cp_x0 = start(x_hbm.at[0], xs.at[0], 1)
    cp_w2 = start(w2_hbm, w2_in, 2)
    cp_w1[1] = start(w1_hbm.at[1], master.at[2], 3)
    cp_t = start(t_hbm, ts, 4)
    cp_x = start(x_hbm.at[pl.ds(1, n_steps - 1)], xs.at[pl.ds(1, n_steps - 1)], 5)

    barrier = pltpu.get_barrier_semaphore()
    for dest in dests:
        pl.semaphore_signal(barrier, inc=1, device_id=dest, device_id_type=MESH)

    def blocks(size):
        return [slice(i, i + size) for i in range(0, batch, size)]

    def norm_of(x):
        return lax.rsqrt(jnp.mean(x * x, axis=-1, keepdims=True) + NORM_EPS)

    def prepare_rows(t, rows):
        x = xs[t, rows, :].astype(F32)
        n_lo[0, rows, :] = (x * norm_of(x)).astype(BF16)

    def prepare(t):
        for rows in blocks(256):
            prepare_rows(t, rows)

    def prepare_tr():
        for rows in blocks(256):
            n_tr[0, :, rows] = n_lo[0, rows, :].T

    def hidden_rows(l, rows, cols, late):
        z = dot(n_lo[l, rows, :], wlo[2 * l, :, cols])
        if late:
            a, d = gelu_value(z), z
        else:
            a, d = gelu_and_slope(z)
        act[l, rows, cols] = a.astype(BF16)
        slope[l, rows, cols] = d

    def hidden_phase(l, cols):
        for rows in blocks(128):
            hidden_rows(l, rows, cols, False)

    def first_half(l, partial):
        for rows in blocks(256):
            partial[rows, :] = dot_rhs_t(act[l, rows, halves[0]], wlo[2 * l + 1, :, halves[0]])

    def product(l, rows, partial):
        if partial is None:
            return dot_rhs_t(act[l, rows, :], wlo[2 * l + 1])
        return partial[rows, :] + dot_rhs_t(act[l, rows, halves[1]], wlo[2 * l + 1, :, halves[1]])

    def out0_rows(t, rows, partial):
        h = (xs[t, rows, :].astype(F32) + product(0, rows, partial)).astype(BF16)
        hid[rows, :] = h
        x = h.astype(F32)
        inv = norm_of(x)
        n = (x * inv).astype(BF16)
        inv_b[rows, :] = jnp.broadcast_to(inv, x.shape)
        n_lo[1, rows, :] = n
        n_tr[1, :, rows] = n.T

    def out1_rows(t, rows, partial):
        loss_scale = 2.0 / (batch * width)
        h = (hid[rows, :].astype(F32) + product(1, rows, partial)).astype(BF16)
        e = loss_scale * (h.astype(F32) - ts[t, rows, :].astype(F32))
        lo = e.astype(BF16)
        err[rows, :] = e
        err_lo[rows, :] = lo
        err_tr[1, :, rows] = lo.T

    def skewed(size, *stages):
        for i in range(batch // size + len(stages) - 1):
            for j, stage in enumerate(stages):
                if 0 <= i - j < batch // size:
                    stage(slice((i - j) * size, (i - j + 1) * size))

    def fine(stage):
        def run(rows):
            for lo in range(rows.start, rows.stop, 128):
                stage(slice(lo, lo + 128))
        return run

    def d_pre_phase(l, cols, late):
        for rows in blocks(512):
            d_act = dot(err_lo[rows, :], wlo[2 * l + 1, :, cols])
            d = slope[l, rows, cols]
            if late:
                d = gelu_and_slope(d)[1]
            dz[l, rows, cols] = (d_act * d).astype(BF16)

    def d_hidden_phase():
        for rows in blocks(512):
            m = dot_rhs_t(dz[1, rows, :], wlo[2])
            inv = inv_b[rows, :]
            n = hid[rows, :].astype(F32) * inv
            e = err[rows, :] + inv * (m - n * jnp.mean(m * n, axis=-1, keepdims=True))
            lo = e.astype(BF16)
            err_lo[rows, :] = lo
            err_tr[0, :, rows] = lo.T

    def update(t, u, left, right, cols):
        q = master[u, :, cols] - LEARN_RATE * dot(left[...], right[:, cols])
        master[u, :, cols] = q
        lo = q.astype(BF16)
        for j in range(0, q.shape[1], part):
            send[t, u * N_PART + (cols.start + j) // part] = lo[:, j:j + part]

    def copy_of(t, d, k):
        return pltpu.make_async_remote_copy(
            src_ref=send.at[t, k], dst_ref=recv.at[t, k, d], send_sem=send_sem.at[0],
            recv_sem=recv_sem.at[t, k], device_id=dests[d], device_id_type=MESH)

    def all_of(ref, sem):
        return pltpu.make_async_remote_copy(
            src_ref=ref, dst_ref=ref, send_sem=sem, recv_sem=sem, device_id=dests[0], device_id_type=MESH)

    def push(t, u, *hs):
        for h in hs:
            for d in range(N_DEST):
                copy_of(t, d, u * N_PART + h).start()

    def combine(t, u, *hs):
        for h in hs:
            k = u * N_PART + h
            all_of(recv.at[t, k], recv_sem.at[t, k]).wait_recv()
            cols = slice(h * part, (h + 1) * part)
            other = recv[t, k, 2].astype(F32)
            total = master[u, :, cols] + recv[t, k, 0].astype(F32) + recv[t, k, 1].astype(F32) + other + other
            p = total / 5.0
            if t < n_steps - 1:
                master[u, :, cols] = p
                wlo[u, :, cols] = p.astype(BF16)
            elif u % 2:
                o2[u // 2, cols, :] = p.T
            else:
                o1[u // 2, :, cols] = p

    everything = slice(0, hidden)
    cp_w1[0].wait()
    wlo[0] = master[0].astype(BF16)
    cp_x0.wait()
    cp_w2.wait()
    w = w2_in[0].T
    master[1] = w
    wlo[1] = w.astype(BF16)

    for t in range(n_steps):
        first = t == 0
        if first:
            skewed(
                SKEW, functools.partial(prepare_rows, 0), fine(lambda rows: hidden_rows(0, rows, everything, True)),
                lambda rows: out0_rows(0, rows, None))
            cp_w1[1].wait()
            wlo[2] = master[2].astype(BF16)
            w = w2_in[1].T
            master[3] = w
            wlo[3] = w.astype(BF16)
            cp_t.wait()
            skewed(SKEW, fine(lambda rows: hidden_rows(1, rows, everything, False)), lambda rows: out1_rows(0, rows, None))
        else:
            combine(t - 1, 3, 0)
            combine(t - 1, 2, 0)
            combine(t - 1, 0, 0)
            hidden_phase(0, halves[0])
            combine(t - 1, 0, 1)
            hidden_phase(0, halves[1])
            combine(t - 1, 1, 0)
            first_half(0, inv_b)
            combine(t - 1, 1, 1)
            for rows in blocks(256):
                out0_rows(t, rows, inv_b)
            hidden_phase(1, halves[0])
            combine(t - 1, 2, 1)
            hidden_phase(1, halves[1])
            combine(t - 1, 3, 1)
            for rows in blocks(256):
                out1_rows(t, rows, None)
        update(t, 3, err_tr.at[1], act.at[1], halves[0])
        if first:
            pl.semaphore_wait(barrier, N_DEST)
        push(t, 3, 0)
        d_pre_phase(1, everything, False)
        update(t, 2, n_tr.at[1], dz.at[1], halves[0])
        push(t, 2, 0)
        d_hidden_phase()
        if first:
            prepare_tr()
        d_pre_phase(0, halves[0], first)
        update(t, 0, n_tr.at[0], dz.at[0], halves[0])
        push(t, 0, 0)
        d_pre_phase(0, halves[1], first)
        update(t, 0, n_tr.at[0], dz.at[0], halves[1])
        push(t, 0, 1)
        update(t, 1, err_tr.at[0], act.at[0], everything)
        push(t, 1, 0, 1)
        update(t, 2, n_tr.at[1], dz.at[1], halves[1])
        push(t, 2, 1)
        update(t, 3, err_tr.at[1], act.at[1], halves[1])
        push(t, 3, 1)
        if first:
            cp_x.wait()
        if t < n_steps - 1:
            prepare(t + 1)
            prepare_tr()

    last = n_steps - 1
    combine(last, 3, 0)
    combine(last, 2, 0)
    combine(last, 0, 0, 1)
    combine(last, 1, 0, 1)
    combine(last, 2, 1)
    combine(last, 3, 1)
    all_of(recv, send_sem.at[0]).wait_send()


def solution(mesh):
    n_rows, n_cols = mesh.shape["row"], mesh.shape["col"]

    def device_fn(w_one, w_two, inputs, targets):
        layers, width, hidden = w_one.shape[2:]
        steps, batch, _ = inputs.shape[2:]
        n_piece = 2 * layers * N_PART
        part = hidden // N_PART
        in_spec = pl.BlockSpec(memory_space=pltpu.HBM)
        out_spec = pl.BlockSpec(memory_space=pltpu.VMEM)
        o1, o2 = pl.pallas_call(
            functools.partial(kernel, n_rows, n_cols),
            out_shape=(jax.ShapeDtypeStruct((layers, width, hidden), F32), jax.ShapeDtypeStruct((layers, hidden, width), F32)),
            in_specs=[in_spec] * 4,
            out_specs=(out_spec, out_spec),
            scratch_shapes=[
                pltpu.VMEM((steps, batch, width), BF16),
                pltpu.VMEM((steps, batch, width), BF16),
                pltpu.VMEM((layers, hidden, width), F32),
                pltpu.VMEM((2 * layers, width, hidden), F32),
                pltpu.VMEM((2 * layers, width, hidden), BF16),
                pltpu.VMEM((layers, batch, hidden), BF16),
                pltpu.VMEM((layers, batch, hidden), F32),
                pltpu.VMEM((layers, batch, width), BF16),
                pltpu.VMEM((layers, width, batch), BF16),
                pltpu.VMEM((batch, width), F32),
                pltpu.VMEM((batch, width), BF16),
                pltpu.VMEM((batch, width), F32),
                pltpu.VMEM((batch, width), BF16),
                pltpu.VMEM((layers, width, batch), BF16),
                pltpu.VMEM((layers, batch, hidden), BF16),
                pltpu.VMEM((steps, n_piece, width, part), BF16),
                pltpu.VMEM((steps, n_piece, N_DEST, width, part), BF16),
                pltpu.SemaphoreType.DMA((6,)),
                pltpu.SemaphoreType.DMA((1,)),
                pltpu.SemaphoreType.DMA((steps, n_piece)),
            ],
            compiler_params=pltpu.CompilerParams(collective_id=0, has_side_effects=True, vmem_limit_bytes=48 * 1024 * 1024),
        )(*[pltpu.with_memory_space_constraint(v[0, 0], pltpu.HBM) for v in (w_one, w_two, inputs, targets)])
        return o1[None, None], o2[None, None]

    grid_spec = P("row", "col")
    return jax.shard_map(device_fn, mesh=mesh, in_specs=(grid_spec,) * 4, out_specs=(grid_spec, grid_spec), check_vma=False)
```

```python
import functools

import jax
import jax.numpy as jnp
from jax import lax
from jax.experimental import pallas as pl
from jax.experimental.pallas import tpu as pltpu
from jax.sharding import PartitionSpec as P

LEARN_RATE = 1.5
NORM_EPS = 1e-6
GELU_C = 0.7978845608028654
GELU_K = 0.044715
MESH = pl.DeviceIdType.MESH
F32 = jnp.float32
BF16 = jnp.bfloat16
N_DEST = 3
SKEW = 512
N_PART = 2


def dot(lhs, rhs):
    return lax.dot_general(lhs, rhs, (((1,), (0,)), ((), ())), preferred_element_type=F32)


def dot_rhs_t(lhs, rhs):
    return lax.dot_general(lhs, rhs, (((1,), (1,)), ((), ())), preferred_element_type=F32)


def gelu_and_slope(z):
    cubic = (GELU_C * GELU_K * z) * z
    th = jnp.tanh(z * (GELU_C + cubic))
    half = 0.5 + 0.5 * th
    act = z * half
    slope = half + act * (1.0 - th) * (GELU_C + 3.0 * cubic)
    return act, slope


def gelu_value(z):
    return z * (0.5 + 0.5 * jnp.tanh(z * (GELU_C + (GELU_C * GELU_K * z) * z)))


def kernel(n_rows, n_cols, w1_hbm, w2_hbm, x_hbm, t_hbm, o1, o2,
           xs, ts, w2_in, master, wlo, act, slope, n_lo, n_tr, inv_b, hid, err, err_lo, err_tr, dz,
           send, recv, in_sem, send_sem, recv_sem):
    n_steps, batch, width = xs.shape
    hidden = act.shape[2]
    part, half = hidden // N_PART, hidden // 2
    halves = [slice(0, half), slice(half, hidden)]
    row, col = lax.axis_index("row"), lax.axis_index("col")
    nxt, prv = lax.rem(col + 1, n_cols), lax.rem(col + n_cols - 1, n_cols)
    dests = ((row, nxt), (row, prv), (lax.rem(row + 1, n_rows), col))

    def start(src, dst, idx):
        cp = pltpu.make_async_copy(src, dst, in_sem.at[idx])
        cp.start()
        return cp

    cp_w1 = [None] * 2
    cp_w1[0] = start(w1_hbm.at[0], master.at[0], 0)
    cp_x0 = start(x_hbm.at[0], xs.at[0], 1)
    cp_w2 = start(w2_hbm, w2_in, 2)
    cp_w1[1] = start(w1_hbm.at[1], master.at[2], 3)
    cp_t = start(t_hbm, ts, 4)
    cp_x = start(x_hbm.at[pl.ds(1, n_steps - 1)], xs.at[pl.ds(1, n_steps - 1)], 5)

    barrier = pltpu.get_barrier_semaphore()
    for dest in dests:
        pl.semaphore_signal(barrier, inc=1, device_id=dest, device_id_type=MESH)

    def blocks(size):
        return [slice(i, i + size) for i in range(0, batch, size)]

    def norm_of(x):
        return lax.rsqrt(jnp.mean(x * x, axis=-1, keepdims=True) + NORM_EPS)

    def prepare_rows(t, rows):
        x = xs[t, rows, :].astype(F32)
        n_lo[0, rows, :] = (x * norm_of(x)).astype(BF16)

    def prepare(t):
        for rows in blocks(256):
            prepare_rows(t, rows)

    def prepare_tr():
        for rows in blocks(256):
            n_tr[0, :, rows] = n_lo[0, rows, :].T

    def hidden_rows(l, rows, cols, late):
        z = dot(n_lo[l, rows, :], wlo[2 * l, :, cols])
        if late:
            a, d = gelu_value(z), z
        else:
            a, d = gelu_and_slope(z)
        act[l, rows, cols] = a.astype(BF16)
        slope[l, rows, cols] = d

    def hidden_phase(l, cols):
        for rows in blocks(128):
            hidden_rows(l, rows, cols, False)

    def first_half(l, partial):
        for rows in blocks(256):
            partial[rows, :] = dot_rhs_t(act[l, rows, halves[0]], wlo[2 * l + 1, :, halves[0]])

    def product(l, rows, partial):
        if partial is None:
            return dot_rhs_t(act[l, rows, :], wlo[2 * l + 1])
        return partial[rows, :] + dot_rhs_t(act[l, rows, halves[1]], wlo[2 * l + 1, :, halves[1]])

    def out0_rows(t, rows, partial):
        h = (xs[t, rows, :].astype(F32) + product(0, rows, partial)).astype(BF16)
        hid[rows, :] = h
        x = h.astype(F32)
        inv = norm_of(x)
        n = (x * inv).astype(BF16)
        inv_b[rows, :] = jnp.broadcast_to(inv, x.shape)
        n_lo[1, rows, :] = n
        n_tr[1, :, rows] = n.T

    def out1_rows(t, rows, partial):
        loss_scale = 2.0 / (batch * width)
        h = (hid[rows, :].astype(F32) + product(1, rows, partial)).astype(BF16)
        e = loss_scale * (h.astype(F32) - ts[t, rows, :].astype(F32))
        lo = e.astype(BF16)
        err[rows, :] = e
        err_lo[rows, :] = lo
        err_tr[1, :, rows] = lo.T

    def skewed(size, *stages):
        for i in range(batch // size + len(stages) - 1):
            for j, stage in enumerate(stages):
                if 0 <= i - j < batch // size:
                    stage(slice((i - j) * size, (i - j + 1) * size))

    def fine(stage):
        def run(rows):
            for lo in range(rows.start, rows.stop, 128):
                stage(slice(lo, lo + 128))
        return run

    def d_pre_phase(l, cols, late):
        for rows in blocks(512):
            d_act = dot(err_lo[rows, :], wlo[2 * l + 1, :, cols])
            d = slope[l, rows, cols]
            if late:
                d = gelu_and_slope(d)[1]
            dz[l, rows, cols] = (d_act * d).astype(BF16)

    def d_hidden_phase():
        for rows in blocks(512):
            m = dot_rhs_t(dz[1, rows, :], wlo[2])
            inv = inv_b[rows, :]
            n = hid[rows, :].astype(F32) * inv
            e = err[rows, :] + inv * (m - n * jnp.mean(m * n, axis=-1, keepdims=True))
            lo = e.astype(BF16)
            err_lo[rows, :] = lo
            err_tr[0, :, rows] = lo.T

    def update(t, u, left, right, cols):
        q = master[u, :, cols] - LEARN_RATE * dot(left[...], right[:, cols])
        master[u, :, cols] = q
        lo = q.astype(BF16)
        for j in range(0, q.shape[1], part):
            send[t, u * N_PART + (cols.start + j) // part] = lo[:, j:j + part]

    def copy_of(t, d, k):
        return pltpu.make_async_remote_copy(
            src_ref=send.at[t, k], dst_ref=recv.at[t, k, d], send_sem=send_sem.at[0],
            recv_sem=recv_sem.at[t, k], device_id=dests[d], device_id_type=MESH)

    def all_of(ref, sem):
        return pltpu.make_async_remote_copy(
            src_ref=ref, dst_ref=ref, send_sem=sem, recv_sem=sem, device_id=dests[0], device_id_type=MESH)

    def push(t, u, *hs):
        for h in hs:
            for d in range(N_DEST):
                copy_of(t, d, u * N_PART + h).start()

    def combine(t, u, *hs):
        for h in hs:
            k = u * N_PART + h
            all_of(recv.at[t, k], recv_sem.at[t, k]).wait_recv()
            cols = slice(h * part, (h + 1) * part)
            other = recv[t, k, 2].astype(F32)
            total = master[u, :, cols] + recv[t, k, 0].astype(F32) + recv[t, k, 1].astype(F32) + other + other
            p = total / 5.0
            if t < n_steps - 1:
                master[u, :, cols] = p
                wlo[u, :, cols] = p.astype(BF16)
            elif u % 2:
                o2[u // 2, cols, :] = p.T
            else:
                o1[u // 2, :, cols] = p

    everything = slice(0, hidden)
    cp_w1[0].wait()
    wlo[0] = master[0].astype(BF16)
    cp_x0.wait()
    cp_w2.wait()
    w = w2_in[0].T
    master[1] = w
    wlo[1] = w.astype(BF16)

    for t in range(n_steps):
        first = t == 0
        if first:
            skewed(
                SKEW, functools.partial(prepare_rows, 0), fine(lambda rows: hidden_rows(0, rows, everything, True)),
                lambda rows: out0_rows(0, rows, None))
            cp_w1[1].wait()
            wlo[2] = master[2].astype(BF16)
            w = w2_in[1].T
            master[3] = w
            wlo[3] = w.astype(BF16)
            cp_t.wait()
            skewed(SKEW, fine(lambda rows: hidden_rows(1, rows, everything, False)), lambda rows: out1_rows(0, rows, None))
        else:
            combine(t - 1, 3, 0)
            combine(t - 1, 2, 0)
            combine(t - 1, 0, 0)
            hidden_phase(0, halves[0])
            combine(t - 1, 0, 1)
            hidden_phase(0, halves[1])
            combine(t - 1, 1, 0)
            first_half(0, inv_b)
            combine(t - 1, 1, 1)
            for rows in blocks(256):
                out0_rows(t, rows, inv_b)
            hidden_phase(1, halves[0])
            combine(t - 1, 2, 1)
            hidden_phase(1, halves[1])
            combine(t - 1, 3, 1)
            for rows in blocks(256):
                out1_rows(t, rows, None)
        update(t, 3, err_tr.at[1], act.at[1], halves[0])
        if first:
            pl.semaphore_wait(barrier, N_DEST)
        push(t, 3, 0)
        d_pre_phase(1, everything, False)
        update(t, 2, n_tr.at[1], dz.at[1], halves[0])
        push(t, 2, 0)
        d_hidden_phase()
        if first:
            prepare_tr()
        d_pre_phase(0, halves[0], first)
        update(t, 0, n_tr.at[0], dz.at[0], halves[0])
        push(t, 0, 0)
        d_pre_phase(0, halves[1], first)
        update(t, 0, n_tr.at[0], dz.at[0], halves[1])
        push(t, 0, 1)
        update(t, 1, err_tr.at[0], act.at[0], everything)
        push(t, 1, 0, 1)
        if t < n_steps - 1:
            update(t, 2, n_tr.at[1], dz.at[1], halves[1])
            push(t, 2, 1)
        update(t, 3, err_tr.at[1], act.at[1], halves[1])
        push(t, 3, 1)
        if t == n_steps - 1:
            update(t, 2, n_tr.at[1], dz.at[1], halves[1])
            push(t, 2, 1)
        if first:
            cp_x.wait()
        if t < n_steps - 1:
            prepare(t + 1)
            prepare_tr()

    last = n_steps - 1
    combine(last, 3, 0)
    combine(last, 2, 0)
    combine(last, 0, 0, 1)
    combine(last, 1, 0, 1)
    combine(last, 3, 1)
    combine(last, 2, 1)
    all_of(recv, send_sem.at[0]).wait_send()


def store(a, b, out_a, out_b, sem):
    copies = [pltpu.make_async_copy(a, out_a, sem.at[0]), pltpu.make_async_copy(b, out_b, sem.at[1])]
    for cp in copies:
        cp.start()
    for cp in copies:
        cp.wait()


def solution(mesh):
    n_rows, n_cols = mesh.shape["row"], mesh.shape["col"]

    def device_fn(w_one, w_two, inputs, targets):
        layers, width, hidden = w_one.shape[2:]
        steps, batch, _ = inputs.shape[2:]
        n_piece = 2 * layers * N_PART
        part = hidden // N_PART
        in_spec = pl.BlockSpec(memory_space=pltpu.HBM)
        out_spec = pl.BlockSpec(memory_space=pltpu.VMEM)
        o1, o2 = pl.pallas_call(
            functools.partial(kernel, n_rows, n_cols),
            out_shape=(jax.ShapeDtypeStruct((layers, width, hidden), F32), jax.ShapeDtypeStruct((layers, hidden, width), F32)),
            in_specs=[in_spec] * 4,
            out_specs=(out_spec, out_spec),
            scratch_shapes=[
                pltpu.VMEM((steps, batch, width), BF16),
                pltpu.VMEM((steps, batch, width), BF16),
                pltpu.VMEM((layers, hidden, width), F32),
                pltpu.VMEM((2 * layers, width, hidden), F32),
                pltpu.VMEM((2 * layers, width, hidden), BF16),
                pltpu.VMEM((layers, batch, hidden), BF16),
                pltpu.VMEM((layers, batch, hidden), F32),
                pltpu.VMEM((layers, batch, width), BF16),
                pltpu.VMEM((layers, width, batch), BF16),
                pltpu.VMEM((batch, width), F32),
                pltpu.VMEM((batch, width), BF16),
                pltpu.VMEM((batch, width), F32),
                pltpu.VMEM((batch, width), BF16),
                pltpu.VMEM((layers, width, batch), BF16),
                pltpu.VMEM((layers, batch, hidden), BF16),
                pltpu.VMEM((steps, n_piece, width, part), BF16),
                pltpu.VMEM((steps, n_piece, N_DEST, width, part), BF16),
                pltpu.SemaphoreType.DMA((6,)),
                pltpu.SemaphoreType.DMA((1,)),
                pltpu.SemaphoreType.DMA((steps, n_piece)),
            ],
            compiler_params=pltpu.CompilerParams(collective_id=0, has_side_effects=True, vmem_limit_bytes=48 * 1024 * 1024),
        )(*[pltpu.with_memory_space_constraint(v[0, 0], pltpu.HBM) for v in (w_one, w_two, inputs, targets)])
        o1, o2 = pl.pallas_call(
            store,
            out_shape=(jax.ShapeDtypeStruct(o1.shape, F32), jax.ShapeDtypeStruct(o2.shape, F32)),
            in_specs=[pl.BlockSpec(memory_space=pl.ANY)] * 2,
            out_specs=(pl.BlockSpec(memory_space=pl.ANY),) * 2,
            scratch_shapes=[pltpu.SemaphoreType.DMA((2,))],
            compiler_params=pltpu.CompilerParams(vmem_limit_bytes=1024 * 1024),
        )(o1, o2)
        return o1[None, None], o2[None, None]

    grid_spec = P("row", "col")
    return jax.shard_map(device_fn, mesh=mesh, in_specs=(grid_spec,) * 4, out_specs=(grid_spec, grid_spec), check_vma=False)
```

```python
import functools

import jax
import jax.numpy as jnp
from jax import lax
from jax.experimental import pallas as pl
from jax.experimental.pallas import tpu as pltpu
from jax.sharding import PartitionSpec as P

LEARN_RATE = 1.5
NORM_EPS = 1e-6
GELU_C = 0.7978845608028654
GELU_K = 0.044715
MESH = pl.DeviceIdType.MESH
F32 = jnp.float32
BF16 = jnp.bfloat16
N_DEST = 3
SKEW = 512
N_PART = 2


def dot(lhs, rhs):
    return lax.dot_general(lhs, rhs, (((1,), (0,)), ((), ())), preferred_element_type=F32)


def dot_rhs_t(lhs, rhs):
    return lax.dot_general(lhs, rhs, (((1,), (1,)), ((), ())), preferred_element_type=F32)


def gelu_and_slope(z):
    cubic = (GELU_C * GELU_K * z) * z
    th = jnp.tanh(z * (GELU_C + cubic))
    half = 0.5 + 0.5 * th
    act = z * half
    slope = half + act * (1.0 - th) * (GELU_C + 3.0 * cubic)
    return act, slope


def gelu_value(z):
    return z * (0.5 + 0.5 * jnp.tanh(z * (GELU_C + (GELU_C * GELU_K * z) * z)))


def kernel(n_rows, n_cols, w1_hbm, w2_hbm, x_hbm, t_hbm, o1, o2,
           xs, ts, w2_in, master, wlo, act, slope, n_lo, n_tr, inv_b, hid, err, err_lo, err_tr, dz,
           send, recv, in_sem, send_sem, recv_sem):
    n_steps, batch, width = xs.shape
    hidden = act.shape[2]
    part, half = hidden // N_PART, hidden // 2
    halves = [slice(0, half), slice(half, hidden)]
    row, col = lax.axis_index("row"), lax.axis_index("col")
    nxt, prv = lax.rem(col + 1, n_cols), lax.rem(col + n_cols - 1, n_cols)
    dests = ((row, nxt), (row, prv), (lax.rem(row + 1, n_rows), col))

    def start(src, dst, idx):
        cp = pltpu.make_async_copy(src, dst, in_sem.at[idx])
        cp.start()
        return cp

    cp_w1 = [None] * 2
    cp_w1[0] = start(w1_hbm.at[0], master.at[0], 0)
    cp_x0 = start(x_hbm.at[0], xs.at[0], 1)
    cp_w2 = start(w2_hbm, w2_in, 2)
    cp_w1[1] = start(w1_hbm.at[1], master.at[2], 3)
    cp_t = start(t_hbm, ts, 4)
    cp_x = start(x_hbm.at[pl.ds(1, n_steps - 1)], xs.at[pl.ds(1, n_steps - 1)], 5)

    barrier = pltpu.get_barrier_semaphore()
    for dest in dests:
        pl.semaphore_signal(barrier, inc=1, device_id=dest, device_id_type=MESH)

    def blocks(size):
        return [slice(i, i + size) for i in range(0, batch, size)]

    def norm_of(x):
        return lax.rsqrt(jnp.mean(x * x, axis=-1, keepdims=True) + NORM_EPS)

    def prepare_rows(t, rows):
        x = xs[t, rows, :].astype(F32)
        n_lo[0, rows, :] = (x * norm_of(x)).astype(BF16)

    def prepare(t):
        for rows in blocks(256):
            prepare_rows(t, rows)

    def prepare_tr():
        for rows in blocks(256):
            n_tr[0, :, rows] = n_lo[0, rows, :].T

    def hidden_rows(l, rows, cols, late):
        z = dot(n_lo[l, rows, :], wlo[2 * l, :, cols])
        if late:
            a, d = gelu_value(z), z
        else:
            a, d = gelu_and_slope(z)
        act[l, rows, cols] = a.astype(BF16)
        slope[l, rows, cols] = d

    def hidden_phase(l, cols):
        for rows in blocks(128):
            hidden_rows(l, rows, cols, False)

    def first_half(l, partial):
        for rows in blocks(256):
            partial[rows, :] = dot_rhs_t(act[l, rows, halves[0]], wlo[2 * l + 1, :, halves[0]])

    def product(l, rows, partial):
        if partial is None:
            return dot_rhs_t(act[l, rows, :], wlo[2 * l + 1])
        return partial[rows, :] + dot_rhs_t(act[l, rows, halves[1]], wlo[2 * l + 1, :, halves[1]])

    def out0_rows(t, rows, partial):
        h = (xs[t, rows, :].astype(F32) + product(0, rows, partial)).astype(BF16)
        hid[rows, :] = h
        x = h.astype(F32)
        inv = norm_of(x)
        n = (x * inv).astype(BF16)
        inv_b[rows, :] = jnp.broadcast_to(inv, x.shape)
        n_lo[1, rows, :] = n
        n_tr[1, :, rows] = n.T

    def out1_rows(t, rows, partial):
        loss_scale = 2.0 / (batch * width)
        h = (hid[rows, :].astype(F32) + product(1, rows, partial)).astype(BF16)
        e = loss_scale * (h.astype(F32) - ts[t, rows, :].astype(F32))
        lo = e.astype(BF16)
        err[rows, :] = e
        err_lo[rows, :] = lo
        err_tr[1, :, rows] = lo.T

    def skewed(size, *stages):
        for i in range(batch // size + len(stages) - 1):
            for j, stage in enumerate(stages):
                if 0 <= i - j < batch // size:
                    stage(slice((i - j) * size, (i - j + 1) * size))

    def fine(stage):
        def run(rows):
            for lo in range(rows.start, rows.stop, 128):
                stage(slice(lo, lo + 128))
        return run

    def d_pre_phase(l, cols, late):
        for rows in blocks(512):
            d_act = dot(err_lo[rows, :], wlo[2 * l + 1, :, cols])
            d = slope[l, rows, cols]
            if late:
                d = gelu_and_slope(d)[1]
            dz[l, rows, cols] = (d_act * d).astype(BF16)

    def d_hidden_phase():
        for rows in blocks(512):
            m = dot_rhs_t(dz[1, rows, :], wlo[2])
            inv = inv_b[rows, :]
            n = hid[rows, :].astype(F32) * inv
            e = err[rows, :] + inv * (m - n * jnp.mean(m * n, axis=-1, keepdims=True))
            lo = e.astype(BF16)
            err_lo[rows, :] = lo
            err_tr[0, :, rows] = lo.T

    def update(t, u, left, right, cols):
        q = master[u, :, cols] - LEARN_RATE * dot(left[...], right[:, cols])
        master[u, :, cols] = q
        lo = q.astype(BF16)
        for j in range(0, q.shape[1], part):
            send[t, u * N_PART + (cols.start + j) // part] = lo[:, j:j + part]

    def copy_of(t, d, k):
        return pltpu.make_async_remote_copy(
            src_ref=send.at[t, k], dst_ref=recv.at[t, k, d], send_sem=send_sem.at[0],
            recv_sem=recv_sem.at[t % 2, k], device_id=dests[d], device_id_type=MESH)

    def all_of(ref, sem):
        return pltpu.make_async_remote_copy(
            src_ref=ref, dst_ref=ref, send_sem=sem, recv_sem=sem, device_id=dests[0], device_id_type=MESH)

    def push(t, u, *hs):
        for h in hs:
            for d in range(N_DEST):
                copy_of(t, d, u * N_PART + h).start()

    def combine(t, u, *hs):
        for h in hs:
            k = u * N_PART + h
            all_of(recv.at[t, k], recv_sem.at[t % 2, k]).wait_recv()
            cols = slice(h * part, (h + 1) * part)
            other = recv[t, k, 2].astype(F32)
            total = master[u, :, cols] + recv[t, k, 0].astype(F32) + recv[t, k, 1].astype(F32) + other + other
            p = total / 5.0
            if t < n_steps - 1:
                master[u, :, cols] = p
                wlo[u, :, cols] = p.astype(BF16)
            elif u % 2:
                o2[u // 2, cols, :] = p.T
            else:
                o1[u // 2, :, cols] = p

    everything = slice(0, hidden)
    cp_w1[0].wait()
    wlo[0] = master[0].astype(BF16)
    cp_x0.wait()
    cp_w2.wait()
    w = w2_in[0].T
    master[1] = w
    wlo[1] = w.astype(BF16)

    for t in range(n_steps):
        first = t == 0
        if first:
            skewed(
                SKEW, functools.partial(prepare_rows, 0), fine(lambda rows: hidden_rows(0, rows, everything, True)),
                lambda rows: out0_rows(0, rows, None))
            cp_w1[1].wait()
            wlo[2] = master[2].astype(BF16)
            w = w2_in[1].T
            master[3] = w
            wlo[3] = w.astype(BF16)
            cp_t.wait()
            skewed(SKEW, fine(lambda rows: hidden_rows(1, rows, everything, False)), lambda rows: out1_rows(0, rows, None))
        else:
            combine(t - 1, 3, 0)
            combine(t - 1, 2, 0)
            combine(t - 1, 0, 0)
            hidden_phase(0, halves[0])
            combine(t - 1, 0, 1)
            hidden_phase(0, halves[1])
            combine(t - 1, 1, 0)
            first_half(0, inv_b)
            combine(t - 1, 1, 1)
            for rows in blocks(256):
                out0_rows(t, rows, inv_b)
            hidden_phase(1, halves[0])
            combine(t - 1, 2, 1)
            hidden_phase(1, halves[1])
            first_half(1, err)
            combine(t - 1, 3, 1)
            for rows in blocks(256):
                out1_rows(t, rows, err)
        update(t, 3, err_tr.at[1], act.at[1], halves[0])
        if first:
            pl.semaphore_wait(barrier, N_DEST)
        push(t, 3, 0)
        d_pre_phase(1, everything, False)
        update(t, 2, n_tr.at[1], dz.at[1], halves[0])
        push(t, 2, 0)
        d_hidden_phase()
        if first:
            prepare_tr()
        d_pre_phase(0, halves[0], first)
        update(t, 0, n_tr.at[0], dz.at[0], halves[0])
        push(t, 0, 0)
        d_pre_phase(0, halves[1], first)
        update(t, 0, n_tr.at[0], dz.at[0], halves[1])
        push(t, 0, 1)
        update(t, 1, err_tr.at[0], act.at[0], everything)
        push(t, 1, 0, 1)
        if t < n_steps - 1:
            update(t, 2, n_tr.at[1], dz.at[1], halves[1])
            push(t, 2, 1)
        update(t, 3, err_tr.at[1], act.at[1], halves[1])
        push(t, 3, 1)
        if t == n_steps - 1:
            update(t, 2, n_tr.at[1], dz.at[1], halves[1])
            push(t, 2, 1)
        if first:
            cp_x.wait()
        if t < n_steps - 1:
            prepare(t + 1)
            prepare_tr()

    last = n_steps - 1
    combine(last, 3, 0)
    combine(last, 2, 0)
    combine(last, 0, 0, 1)
    combine(last, 1, 0, 1)
    combine(last, 3, 1)
    combine(last, 2, 1)
    all_of(recv, send_sem.at[0]).wait_send()


def store(a, b, out_a, out_b, sem):
    copies = [pltpu.make_async_copy(a, out_a, sem.at[0]), pltpu.make_async_copy(b, out_b, sem.at[1])]
    for cp in copies:
        cp.start()
    for cp in copies:
        cp.wait()


def solution(mesh):
    n_rows, n_cols = mesh.shape["row"], mesh.shape["col"]

    def device_fn(w_one, w_two, inputs, targets):
        layers, width, hidden = w_one.shape[2:]
        steps, batch, _ = inputs.shape[2:]
        n_piece = 2 * layers * N_PART
        part = hidden // N_PART
        in_spec = pl.BlockSpec(memory_space=pltpu.HBM)
        out_spec = pl.BlockSpec(memory_space=pltpu.VMEM)
        o1, o2 = pl.pallas_call(
            functools.partial(kernel, n_rows, n_cols),
            out_shape=(jax.ShapeDtypeStruct((layers, width, hidden), F32), jax.ShapeDtypeStruct((layers, hidden, width), F32)),
            in_specs=[in_spec] * 4,
            out_specs=(out_spec, out_spec),
            scratch_shapes=[
                pltpu.VMEM((steps, batch, width), BF16),
                pltpu.VMEM((steps, batch, width), BF16),
                pltpu.VMEM((layers, hidden, width), F32),
                pltpu.VMEM((2 * layers, width, hidden), F32),
                pltpu.VMEM((2 * layers, width, hidden), BF16),
                pltpu.VMEM((layers, batch, hidden), BF16),
                pltpu.VMEM((layers, batch, hidden), F32),
                pltpu.VMEM((layers, batch, width), BF16),
                pltpu.VMEM((layers, width, batch), BF16),
                pltpu.VMEM((batch, width), F32),
                pltpu.VMEM((batch, width), BF16),
                pltpu.VMEM((batch, width), F32),
                pltpu.VMEM((batch, width), BF16),
                pltpu.VMEM((layers, width, batch), BF16),
                pltpu.VMEM((layers, batch, hidden), BF16),
                pltpu.VMEM((steps, n_piece, width, part), BF16),
                pltpu.VMEM((steps, n_piece, N_DEST, width, part), BF16),
                pltpu.SemaphoreType.DMA((6,)),
                pltpu.SemaphoreType.DMA((1,)),
                pltpu.SemaphoreType.DMA((2, n_piece)),
            ],
            compiler_params=pltpu.CompilerParams(collective_id=0, has_side_effects=True, vmem_limit_bytes=48 * 1024 * 1024),
        )(*[pltpu.with_memory_space_constraint(v[0, 0], pltpu.HBM) for v in (w_one, w_two, inputs, targets)])
        o1, o2 = pl.pallas_call(
            store,
            out_shape=(jax.ShapeDtypeStruct(o1.shape, F32), jax.ShapeDtypeStruct(o2.shape, F32)),
            in_specs=[pl.BlockSpec(memory_space=pl.ANY)] * 2,
            out_specs=(pl.BlockSpec(memory_space=pl.ANY),) * 2,
            scratch_shapes=[pltpu.SemaphoreType.DMA((2,))],
            compiler_params=pltpu.CompilerParams(vmem_limit_bytes=1024 * 1024),
        )(o1, o2)
        return o1[None, None], o2[None, None]

    grid_spec = P("row", "col")
    return jax.shard_map(device_fn, mesh=mesh, in_specs=(grid_spec,) * 4, out_specs=(grid_spec, grid_spec), check_vma=False)
```
